32 devices in a mesh: rows: 8 (over z, x), cols: 4 (over y, core).
Axes of the slice: x: 2, y: 2, z: 4, core: 2. Of those that a mesh axis runs over, the one named last changes fastest.
Arguments:
- coupling: float32 [2, 16384, 16384], P(None, 'rows', 'cols'), may hold values from -2 to 40, as said below
- initial: float32 [2, 48, 16384], P(None, None, 'rows'), may hold values from -8 to 8
Outputs:
- basis: float32 [2, 48, 16384], P(None, None, ('rows', 'cols'))
- ritz: float32 [4, 2, 48, 48], replicated
The draws below stay inside these ranges and needn't reach their ends.
Inputs may be any that keep to these rules, and one draw needn't show every extreme that they name: `coupling`: H is Hermitian (the first plane symmetric, the second antisymmetric) and positive definite.
All inputs are finite; a program needn't handle non-finite values.
Results may differ from the reference program's by a relative error of at most 0.0003.
Values sent between devices are 32-bit elements; how exact they have to be, the bound alone decides.
No kernel may reach another device: no remote copies, remote signals or barrier semaphores. Data moves between devices by JAX's collectives and lax.ppermute only.
A program may use at most 128 MiB of HBM per device.

```python
import jax
import jax.numpy as jnp
from jax import lax

N = 16384
K = 48
ITERS = 4


def draw_coupling(key, part):
    first, second, third, fourth = jax.random.split(jax.random.fold_in(key, 7), 4)
    scales = jax.random.uniform(third, (N,), minval=0.8, maxval=1.25)
    outer = scales[:, None] * scales[None, :]
    shifts = 4.5 + 1.5 * jax.random.uniform(fourth, (N,))
    index = jnp.arange(N, dtype=jnp.int32)
    partner = (index + N // 2) % N
    band = (index[None, :] == partner[:, None]).astype(jnp.float32)
    noise = jax.random.normal(first, (N, N), jnp.float32)
    real_plane = (noise + noise.T) * (0.5 / jnp.sqrt(N * 1.0))
    real_plane = (real_plane + band + jnp.diag(shifts)) * outer
    noise = jax.random.normal(second, (N, N), jnp.float32)
    imag_plane = (noise - noise.T) * (0.5 / jnp.sqrt(N * 1.0)) * outer
    return jnp.stack([real_plane, imag_plane])


def draw_initial(key, part):
    inner = jax.random.fold_in(key, 11)
    position = jnp.arange(N, dtype=jnp.float32) / N
    amplitude = 3.0 ** (0.5 * (position - 0.5))
    values = jnp.clip(jax.random.normal(inner, (2, K, N), jnp.float32), -6.0, 6.0)
    return values * amplitude[None, None, :]


def setup_inputs(seed: int = 0) -> dict:
    key_list = jax.random.split(jax.random.key(seed), 3)
    coupling = draw_coupling(jax.random.fold_in(key_list[2], 71), 0)
    initial = draw_initial(jax.random.fold_in(key_list[2], 71), 0)
    return dict(coupling=coupling, initial=initial)


HIGH = lax.Precision.HIGHEST

def pair_products(left, right):
    real_part = jnp.dot(left[0], right[0].T, precision=HIGH) + jnp.dot(left[1], right[1].T, precision=HIGH)
    imag_part = jnp.dot(left[0], right[1].T, precision=HIGH) - jnp.dot(left[1], right[0].T, precision=HIGH)
    return jnp.stack([real_part, imag_part])

def orthonormal(gram_matrix, images):
    gram_re = gram_matrix[0]
    gram_im = gram_matrix[1]
    vectors = gram_re.shape[0]
    width = images.shape[2]
    upper_pair = jnp.stack([gram_re, -gram_im], axis=-1)
    lower_pair = jnp.stack([gram_im, gram_re], axis=-1)
    embedded = jnp.stack([upper_pair, lower_pair], axis=1).reshape(2 * vectors, 2 * vectors)
    factor = jnp.linalg.cholesky(embedded)
    woven = jnp.transpose(images, (1, 0, 2)).reshape(2 * vectors, width)
    solved = lax.linalg.triangular_solve(factor, woven, left_side=True, lower=True)
    return jnp.transpose(solved.reshape(vectors, 2, width), (1, 0, 2))

def reference(coupling, initial):
    contract = (((1,), (1,)), ((), ()))
    current = initial
    ritz_list = []
    for iteration in range(ITERS):
        stacked = current.reshape(2 * K, N)
        with_real = lax.dot_general(stacked.astype(jnp.float32), coupling[0].astype(jnp.float32), contract, precision=HIGH, preferred_element_type=jnp.float32)
        with_imag = lax.dot_general(stacked.astype(jnp.float32), coupling[1].astype(jnp.float32), contract, precision=HIGH, preferred_element_type=jnp.float32)
        images = jnp.stack([with_real[:K] - with_imag[K:], with_real[K:] + with_imag[:K]])
        gram_matrix = pair_products(images, images) / N
        ritz_list.append(pair_products(current, images) / N)
        current = orthonormal(gram_matrix, images)
    return (current, jnp.stack(ritz_list))
```

```python
import functools

import jax
import jax.numpy as jnp
from jax import lax
from jax.experimental import pallas as pl
from jax.experimental.pallas import tpu as pltpu
from jax.sharding import PartitionSpec as P


F32 = jnp.float32
BF16 = jnp.bfloat16
LANES = 128
TILE = (256, 1024)
DEPTH = 8
CHUNKS = 2
ANY = pl.BlockSpec(memory_space=pl.ANY)
NT = (((1,), (1,)), ((), ()))
NN = (((1,), (0,)), ((), ()))


def split(value):
    high = value.astype(BF16)
    return high, (value - high.astype(F32)).astype(BF16)


def mul(left, right, dims):
    return lax.dot_general(left, right, dims, preferred_element_type=F32)


def triple(left, right, dims):
    left_high, left_low = split(left)
    right_high, right_low = split(right)
    return (
        mul(left_high, right_high, dims)
        + mul(left_low, right_high, dims)
        + mul(left_high, right_low, dims)
    )


def twisted(value, half, sign):
    return jnp.concatenate([sign * value[half:], -sign * value[:half]], axis=0)


def pairs(left, right, half):
    full = mul(left, right, NT)
    rows = 2 * half
    full = full[:rows, :rows] + full[:rows, rows:] + full[rows:, :rows]
    real = full[:half, :half] + full[half:, half:]
    imag = full[:half, half:] - full[half:, :half]
    gap = jnp.zeros((half, LANES // 2 - half), F32)
    return jnp.concatenate([real, gap, imag, gap], axis=1)


def block_product(matrix, real_factor, imag_factor, dims):
    rows = real_factor.shape[0] // 2
    real_high, real_low = split(matrix[0])
    imag_high, imag_low = split(matrix[1])
    both = mul(real_factor, real_high, dims) + mul(imag_factor, imag_high, dims)
    low = mul(real_factor[:rows], real_low, dims) + mul(imag_factor[:rows], imag_low, dims)
    return both[:rows] + both[rows:] + low


def stack_split(value):
    high, low = split(value)
    return jnp.concatenate([high, low], axis=0)


def whole_spec(shape):
    return pl.BlockSpec(shape, lambda *_: (0,) * len(shape))


def offsets(bits):
    result = [0]
    for bit in bits:
        result += [k + bit for k in result]
    return sorted(result, key=lambda k: [bool(k & bit) for bit in bits])


def exchange(value, axis, step):
    count = lax.axis_size(axis)
    return lax.ppermute(value, axis, [(i, i ^ step) for i in range(count)])


def bits_of(count):
    return [1 << t for t in range(count.bit_length() - 1)]


class Stream:
    def __init__(self, matrix, buffer, sems, window, steps):
        self.matrix, self.buffer, self.sems = matrix, buffer, sems
        self.window, self.steps, self.depth = window, steps, buffer.shape[0]
        self.shape = buffer.shape[2:]

    def copy(self, step):
        row, column = self.window(step)
        slot = lax.rem(step, self.depth) if not isinstance(step, int) else step % self.depth
        rows, columns = self.shape
        if not isinstance(step, int):
            row, column = pl.multiple_of(row, rows), pl.multiple_of(column, LANES)
        source = self.matrix.at[:, pl.ds(row, rows), pl.ds(column, columns)]
        return pltpu.make_async_copy(source, self.buffer.at[slot], self.sems.at[slot])

    def begin(self):
        for step in range(min(self.depth, self.steps)):
            self.copy(step).start()

    def run(self, compute):
        @pl.loop(0, self.steps)
        def _(step):
            self.copy(step).wait()
            compute(step, self.buffer.at[lax.rem(step, self.depth)])

            @pl.when(step + self.depth < self.steps)
            def _():
                self.copy(step + self.depth).start()


def ring(tile, count):
    depth = min(DEPTH, count)
    return [pltpu.VMEM((depth, 2, *tile), F32), pltpu.SemaphoreType.DMA((depth,))]


def first_factor(vectors, half):
    rows, width = vectors.shape

    def kernel(v_ref, real_ref, imag_ref):
        value = v_ref[...]
        real_ref[...] = stack_split(value)
        imag_ref[...] = stack_split(twisted(value, half, 1.0))

    shape = jax.ShapeDtypeStruct((2 * rows, width), BF16)
    return pl.pallas_call(kernel, out_shape=(shape, shape), name="first_factor")(vectors)


def column_product(coupling, real_factor, imag_factor, chunk, width, bits):
    double, height = real_factor.shape
    rows = double // 2
    order = offsets(bits)
    members = len(order)
    piece = width // members
    tile = (min(TILE[0], height), min(TILE[1], width))
    down, along = height // tile[0], width // tile[1]
    steps = down * along

    def kernel(h_ref, real_ref, imag_ref, near_ref, far_ref, total, pieces, buffer, sems):
        def window(step):
            return (step % down) * tile[0], chunk * width + (step // down) * tile[1]

        stream = Stream(h_ref, buffer, sems, window, steps)
        stream.begin()
        total[...] = jnp.zeros_like(total)

        def compute(step, matrix):
            inner = pl.ds(pl.multiple_of(lax.rem(step, down) * tile[0], tile[0]), tile[0])
            outer = pl.ds(pl.multiple_of(lax.div(step, down) * tile[1], tile[1]), tile[1])
            total[:, outer] += block_product(matrix, real_ref[:, inner], imag_ref[:, inner], NN)

        stream.run(compute)
        mine = lax.axis_index("rows")
        for p in range(members):
            pieces[p] = total[:, p * piece : (p + 1) * piece]
        for e in range(members // 2):
            near_ref[e] = pieces[mine ^ order[e]]
            far_ref[e] = pieces[mine ^ order[members // 2 + e]]

    out = jax.ShapeDtypeStruct((members // 2, rows, piece), F32)
    vmem = pl.BlockSpec(memory_space=pltpu.VMEM)
    return pl.pallas_call(
        kernel,
        in_specs=[ANY, vmem, vmem],
        out_shape=[out, out],
        scratch_shapes=[
            pltpu.VMEM((rows, width), F32),
            pltpu.VMEM((members, rows, piece), F32),
            *ring(tile, steps),
        ],
        name="column_product",
        cost_estimate=pl.CostEstimate(
            flops=4 * 3 * rows * height * width,
            bytes_accessed=8 * height * width,
            transcendentals=0,
        ),
    )(coupling, real_factor, imag_factor)


def sum_all(parts):
    return functools.reduce(jnp.add, parts)


def row_product(coupling, parts, bits, inverse, before, carry, chunk, width, geometry):
    rows_axis, cols_axis, chunks = geometry
    order = offsets(bits)
    _, rows, piece = parts[0].shape
    half = rows // 2
    height = before.shape[1]
    first, last = carry is None, chunk == chunks - 1
    normal = inverse is not None
    start = chunk * width
    owner_row, offset = start // height, start % height
    kept = height // cols_axis
    per_chunk = width // kept
    ratio = rows_axis // cols_axis
    tile = (min(TILE[0], height), min(TILE[1], width))
    down, along = height // tile[0], width // tile[1]
    steps = down * along
    n_sum = 2 if last else 1

    def kernel(*refs):
        refs = list(refs)
        h_ref = refs.pop(0)
        part_refs = [refs.pop(0) for _ in parts]
        inverse_ref = refs.pop(0) if normal else None
        before_ref = refs.pop(0)
        carry_refs = None if first else [refs.pop(0) for _ in range(4)]
        sum_refs = [refs.pop(0) for _ in range(n_sum)]
        gram_ref, cross_ref, keep_ref, vector_ref = (refs.pop(0) for _ in range(4))
        real_factor, imag_factor, pieces, buffer, sems = (refs.pop(0) for _ in range(5))
        total, out_pieces = (refs.pop(0), refs.pop(0)) if last else (sum_refs[0], None)
        row, column = lax.axis_index("rows"), lax.axis_index("cols")

        def window(step):
            return (step // along) * tile[0], start + (step % along) * tile[1]

        stream = Stream(h_ref, buffer, sems, window, steps)
        stream.begin()
        split_at = len(order) // len(parts)
        for e, k in enumerate(order):
            pieces[row ^ k] = part_refs[e // split_at][e % split_at]
        value = jnp.concatenate([pieces[p] for p in range(rows_axis)], axis=1)
        if normal:
            value = triple(inverse_ref[...], value, NN)
        vector_ref[...] = value
        factor = stack_split(value)
        real_factor[...] = factor
        imag_factor[...] = stack_split(twisted(value, half, -1.0))
        gram = pairs(factor, factor, half)
        ours = (row == column * ratio + owner_row).astype(F32)
        earlier = stack_split(before_ref[:, offset : offset + width])
        cross = pairs(earlier, factor, half) * ours
        gram_ref[...] = gram if first else carry_refs[1][...] + gram
        cross_ref[...] = cross if first else carry_refs[2][...] + cross
        keep_ref[...] = jnp.zeros_like(keep_ref) if first else carry_refs[3][...]
        for p in range(per_chunk):

            @pl.when(row == chunk * per_chunk + p)
            def _(p=p):
                keep_ref[...] = vector_ref[:, p * kept : (p + 1) * kept]

        total[...] = jnp.zeros_like(total) if first else carry_refs[0][...]

        def compute(step, matrix):
            inner = pl.ds(pl.multiple_of(lax.rem(step, along) * tile[1], tile[1]), tile[1])
            outer = pl.ds(pl.multiple_of(lax.div(step, along) * tile[0], tile[0]), tile[0])
            total[:, outer] += block_product(matrix, real_factor[:, inner], imag_factor[:, inner], NT)

        stream.run(compute)
        if last:
            for p in range(cols_axis):
                out_pieces[p] = total[:, p * kept : (p + 1) * kept]
            for e in range(cols_axis // 2):
                sum_refs[0][e] = out_pieces[column ^ (2 * e)]
                sum_refs[1][e] = out_pieces[column ^ (2 * e + 1)]

    small = jax.ShapeDtypeStruct((half, LANES), F32)
    pair = jax.ShapeDtypeStruct((cols_axis // 2, rows, kept), F32)
    out_shape = [pair, pair] if last else [jax.ShapeDtypeStruct((rows, height), F32)]
    out_shape += [
        small,
        small,
        jax.ShapeDtypeStruct((rows, kept), F32),
        jax.ShapeDtypeStruct((rows, width), F32),
    ]
    scratch = [
        pltpu.VMEM((2 * rows, width), BF16),
        pltpu.VMEM((2 * rows, width), BF16),
        pltpu.VMEM((rows_axis, rows, piece), F32),
        *ring(tile, steps),
    ]
    if last:
        scratch += [pltpu.VMEM((rows, height), F32), pltpu.VMEM((cols_axis, rows, kept), F32)]
    operands = [*parts]
    operands += [inverse] if normal else []
    operands += [before]
    operands += [] if first else list(carry)
    outs = pl.pallas_call(
        kernel,
        in_specs=[ANY] + [pl.BlockSpec(memory_space=pltpu.VMEM)] * len(operands),
        out_shape=out_shape,
        scratch_shapes=scratch,
        name="row_product",
        cost_estimate=pl.CostEstimate(
            flops=4 * 3 * rows * height * width,
            bytes_accessed=8 * height * width,
            transcendentals=0,
        ),
    )(coupling, *operands)
    sums, (gram, cross, keep, vectors) = outs[:n_sum], outs[n_sum:]
    return (sums if last else sums[0], gram, cross, keep), vectors


def inverse_factor(parts, count, order):
    total_rows = parts[0].shape[0]
    middle = LANES // 2
    rest = total_rows - count

    def kernel(*refs):
        ins, outs = refs[: len(parts)], refs[len(parts) :]
        total = sum_all([ref[...] for ref in ins])
        if rest:
            outs[1][...] = total[count:]
        gram = total[:count] * (1.0 / order)
        lane = lax.broadcasted_iota(jnp.int32, (count, LANES), 1)
        row = lax.broadcasted_iota(jnp.int32, (count, LANES), 0)
        left = lane < count
        identity = (lane == row + middle).astype(F32)
        real = jnp.where(left, gram, identity)
        imag = jnp.where(left, pltpu.roll(gram, middle, 1), 0.0)
        row_column = lax.broadcasted_iota(jnp.int32, (count, 1), 0)
        scale = jnp.zeros((count, 1), F32)
        for j in range(count):
            pivot = real[j : j + 1, j : j + 1]
            scale = jnp.where(row_column == j, lax.rsqrt(pivot), scale)
            if j == count - 1:
                break
            top = (j + 1) // 8 * 8
            below = row_column[top:] > j
            gain = 1.0 / pivot
            column_real = jnp.where(below, real[top:, j : j + 1] * gain, 0.0)
            column_imag = jnp.where(below, imag[top:, j : j + 1] * gain, 0.0)
            row_real, row_imag = real[j : j + 1], imag[j : j + 1]
            new_real = real[top:] - (column_real * row_real - column_imag * row_imag)
            new_imag = imag[top:] - (column_real * row_imag + column_imag * row_real)
            real = jnp.concatenate([real[:top], new_real], axis=0) if top else new_real
            imag = jnp.concatenate([imag[:top], new_imag], axis=0) if top else new_imag
        real = (real * scale)[:, middle : middle + count]
        imag = (imag * scale)[:, middle : middle + count]
        outs[0][...] = jnp.concatenate(
            [
                jnp.concatenate([real, -imag], axis=1),
                jnp.concatenate([imag, real], axis=1),
            ],
            axis=0,
        )

    out_shape = [jax.ShapeDtypeStruct((2 * count, 2 * count), F32)]
    if rest:
        out_shape.append(jax.ShapeDtypeStruct((rest, LANES), F32))
    outs = pl.pallas_call(kernel, out_shape=out_shape, name="inverse_factor")(*parts)
    return (outs[0], outs[1] if rest else None)


def next_factor(own, inverse, earlier, geometry):
    rows_axis, cols_axis, chunks = geometry
    _, rows, kept = own[0][0].shape
    half = rows // 2
    height = kept * cols_axis
    width = earlier[0].shape[1]
    ratio = rows_axis // cols_axis
    counts = [len(terms) for terms in own]
    flat = [term for terms in own for term in terms]

    def kernel(*refs):
        refs = list(refs)
        term_refs = [[refs.pop(0) for _ in range(n)] for n in counts]
        inverse_ref = refs.pop(0)
        earlier_refs = [refs.pop(0) for _ in range(chunks)]
        real_ref, imag_ref, value_ref, gram_ref, cross_ref, pieces, packed = refs
        row, column = lax.axis_index("rows"), lax.axis_index("cols")
        for k in range(cols_axis):
            terms = [ref[(k // 2) ^ m] for m, ref in enumerate(term_refs[k % 2])]
            pieces[column ^ k] = sum_all(terms)
        value = jnp.concatenate([pieces[p] for p in range(cols_axis)], axis=1)
        value = triple(inverse_ref[...], value, NN)
        value_ref[...] = value
        factor = stack_split(value)
        packed[...] = factor
        real_ref[...] = factor
        imag_ref[...] = stack_split(twisted(value, half, 1.0))
        gram_ref[...] = pairs(factor, factor, half)
        cross_ref[...] = jnp.zeros_like(cross_ref)
        for j in range(chunks):
            owner, offset = j * width // height, j * width % height

            @pl.when(row == column * ratio + owner)
            def _(j=j, offset=offset):
                cross_ref[...] += pairs(
                    stack_split(earlier_refs[j][...]),
                    packed[:, offset : offset + width],
                    half,
                )

    factor_shape = jax.ShapeDtypeStruct((2 * rows, height), BF16)
    small_shape = jax.ShapeDtypeStruct((half, LANES), F32)
    return pl.pallas_call(
        kernel,
        out_shape=[
            factor_shape,
            factor_shape,
            jax.ShapeDtypeStruct((rows, height), F32),
            small_shape,
            small_shape,
        ],
        scratch_shapes=[
            pltpu.VMEM((cols_axis, rows, kept), F32),
            pltpu.VMEM((2 * rows, height), BF16),
        ],
        name="next_factor",
    )(*flat, inverse, *earlier)


def last_vectors(terms, inverse, earlier):
    rows, kept = terms[0].shape
    half = rows // 2

    def kernel(*refs):
        ins, (inverse_ref, earlier_ref, value_ref, both_ref) = refs[: len(terms)], refs[len(terms) :]
        value = triple(inverse_ref[...], sum_all([ref[...] for ref in ins]), NN)
        value_ref[...] = value
        factor = stack_split(value)
        both_ref[:half] = pairs(factor, factor, half)
        both_ref[half:] = pairs(stack_split(earlier_ref[...]), factor, half)

    return pl.pallas_call(
        kernel,
        out_shape=[
            jax.ShapeDtypeStruct((rows, kept), F32),
            jax.ShapeDtypeStruct((2 * half, LANES), F32),
        ],
        name="last_vectors",
    )(*terms, inverse, earlier)


def finish(value, inverse, crosses, inverses, order):
    rows, kept = value.shape
    half = rows // 2
    middle = LANES // 2
    count = len(crosses)

    def kernel(*refs):
        value_ref, inverse_ref = refs[:2]
        cross_refs, inverse_refs = refs[2 : 2 + count], refs[2 + count : 1 + 2 * count]
        basis_ref, ritz_ref = refs[1 + 2 * count :]
        result = triple(inverse_ref[...], value_ref[...], NN)
        basis_ref[0], basis_ref[1] = result[:half], result[half:]
        for t in range(count):
            cross = cross_refs[t][...] * (1.0 / order)
            stacked = jnp.concatenate(
                [cross[:, :half], cross[:, middle : middle + half]], axis=0
            )
            if t:
                factor = inverse_refs[t - 1][...]
                conjugate = jnp.concatenate(
                    [
                        jnp.concatenate([factor[:half, :half], -factor[:half, half:]], axis=1),
                        jnp.concatenate([-factor[half:, :half], factor[half:, half:]], axis=1),
                    ],
                    axis=0,
                )
                stacked = triple(conjugate, stacked, NN)
            ritz_ref[t, 0], ritz_ref[t, 1] = stacked[:half], stacked[half:]

    return pl.pallas_call(
        kernel,
        out_shape=[
            jax.ShapeDtypeStruct((2, half, kept), F32),
            jax.ShapeDtypeStruct((count, 2, half, half), F32),
        ],
        name="finish",
    )(value, inverse, *crosses, *inverses)


def body(coupling, initial):
    rows_axis, cols_axis = lax.axis_size("rows"), lax.axis_size("cols")
    half = initial.shape[1]
    rows = 2 * half
    height, span = coupling.shape[1], coupling.shape[2]
    order = float(height * rows_axis)
    ratio = rows_axis // cols_axis
    chunks = max(ratio, CHUNKS)
    width = span // chunks
    geometry = (rows_axis, cols_axis, chunks)
    row_bits, col_bits = bits_of(rows_axis), bits_of(cols_axis)
    orders = [row_bits if chunk % 2 == 0 else row_bits[1:] + row_bits[:1] for chunk in range(chunks)]

    def tie(value, after):
        return lax.optimization_barrier((value, after))

    def forward(real_factor, imag_factor, small):
        steps = list(row_bits)
        products = []
        for chunk in range(chunks):
            if small is not None and steps:
                away = exchange(small, "rows", steps.pop(0))
            else:
                away = None
            products.append(
                column_product(coupling, real_factor, imag_factor, chunk, width, orders[chunk])
            )
            if away is not None:
                small = small + away
                real_factor, small = tie(real_factor, small)
        gathered = []
        for (near, far), bits in zip(products, orders):
            for bit in bits:
                came = exchange(far, "rows", bit)
                middle = near.shape[0] // 2
                if middle:
                    near, far = near[:middle] + came[:middle], near[middle:] + came[middle:]
                else:
                    near = near + came
            for bit in bits[:0:-1]:
                near = jnp.concatenate([near, exchange(near, "rows", bit)], axis=0)
            gathered.append([near, exchange(near, "rows", bits[0])])
        while small is not None and steps:
            small = small + exchange(small, "rows", steps.pop(0))
        return gathered, small

    def backward(gathered, inverse, before):
        carry, vectors = None, []
        for chunk in range(chunks):
            carry, value = row_product(
                coupling, gathered[chunk], orders[chunk], inverse, before, carry, chunk, width, geometry
            )
            vectors.append(value)
        return carry, vectors

    def total(value, axis, bits):
        for bit in bits:
            value = value + exchange(value, axis, bit)
        return value

    start = initial.reshape(rows, height)
    real_factor, imag_factor = first_factor(start, half)
    others = range(2, cols_axis, 2)
    gathered, _ = forward(real_factor, imag_factor, None)
    ((near, far), gram, cross_1, _), vectors = backward(gathered, None, start)
    near = near + exchange(far, "cols", 1)
    across = [near] + [exchange(near, "cols", m) for m in others]
    packed = total(jnp.concatenate([gram, cross_1], axis=0), "cols", col_bits)
    inverse_1, cross_1 = inverse_factor([packed], half, order)
    own = [across, [exchange(term, "cols", 1) for term in across]]
    real_factor, imag_factor, before, gram, cross_2 = next_factor(own, inverse_1, vectors, geometry)
    packed = jnp.concatenate([gram, cross_2, cross_1], axis=0)
    gathered, packed = forward(real_factor, imag_factor, packed)
    inverse_2, crosses = inverse_factor([packed], half, order)
    cross_2, cross_1 = crosses[:half], crosses[half:]
    ((near, far), gram, cross_3, keep), _ = backward(gathered, inverse_2, before)
    near = near + exchange(far, "cols", 1)
    keep = lax.ppermute(
        keep,
        ("rows", "cols"),
        [
            (r * cols_axis + c, (c * ratio + r // cols_axis) * cols_axis + r % cols_axis)
            for r in range(rows_axis)
            for c in range(cols_axis)
        ],
    )
    terms = [near[0]] + [exchange(near[m // 2], "cols", m) for m in others]
    packed = total(jnp.concatenate([gram, cross_3, cross_2], axis=0), "cols", col_bits)
    inverse_3, crosses = inverse_factor([packed], half, order)
    cross_3, cross_2 = crosses[:half], crosses[half:]
    value, both = last_vectors(terms, inverse_3, keep)
    both = total(both, "cols", col_bits)
    packed = total(jnp.concatenate([both, cross_3], axis=0), "rows", row_bits)
    inverse_4, crosses = inverse_factor([packed], half, order)
    cross_4, cross_3 = crosses[:half], crosses[half:]
    return tuple(
        finish(
            value,
            inverse_4,
            [cross_1, cross_2, cross_3, cross_4],
            [inverse_1, inverse_2, inverse_3],
            order,
        )
    )


def solution(mesh):
    return jax.shard_map(
        body,
        mesh=mesh,
        in_specs=(P(None, "rows", "cols"), P(None, None, "rows")),
        out_specs=(P(None, None, ("rows", "cols")), P()),
        check_vma=False,
    )
```

```python
import functools

import jax
import jax.numpy as jnp
from jax import lax
from jax.experimental import pallas as pl
from jax.experimental.pallas import tpu as pltpu
from jax.sharding import PartitionSpec as P


F32 = jnp.float32
BF16 = jnp.bfloat16
LANES = 128
COLUMN_TILE = (512, 1024)
ROW_TILE = (256, 2048)
DEPTH = 4
CHUNKS = 2
ANY = pl.BlockSpec(memory_space=pl.ANY)
NT = (((1,), (1,)), ((), ()))
NN = (((1,), (0,)), ((), ()))


def split(value):
    high = value.astype(BF16)
    return high, (value - high.astype(F32)).astype(BF16)


def mul(left, right, dims):
    return lax.dot_general(left, right, dims, preferred_element_type=F32)


def triple(left, right, dims):
    left_high, left_low = split(left)
    right_high, right_low = split(right)
    return (
        mul(left_high, right_high, dims)
        + mul(left_low, right_high, dims)
        + mul(left_high, right_low, dims)
    )


def twisted(value, half, sign):
    return jnp.concatenate([sign * value[half:], -sign * value[:half]], axis=0)


def pairs(left, right, half):
    full = mul(left, right, NT)
    rows = 2 * half
    full = full[:rows, :rows] + full[:rows, rows:] + full[rows:, :rows]
    real = full[:half, :half] + full[half:, half:]
    imag = full[:half, half:] - full[half:, :half]
    gap = jnp.zeros((half, LANES // 2 - half), F32)
    return jnp.concatenate([real, gap, imag, gap], axis=1)


def block_product(matrix, real_factor, imag_factor, dims):
    rows = real_factor.shape[0] // 2
    real_high, real_low = split(matrix[0])
    imag_high, imag_low = split(matrix[1])
    both = mul(real_factor, real_high, dims) + mul(imag_factor, imag_high, dims)
    low = mul(real_factor[:rows], real_low, dims) + mul(imag_factor[:rows], imag_low, dims)
    return both[:rows] + both[rows:] + low


def stack_split(value):
    high, low = split(value)
    return jnp.concatenate([high, low], axis=0)


def whole_spec(shape):
    return pl.BlockSpec(shape, lambda *_: (0,) * len(shape))


def offsets(bits):
    result = [0]
    for bit in bits:
        result += [k + bit for k in result]
    return sorted(result, key=lambda k: [bool(k & bit) for bit in bits])


def exchange(value, axis, step):
    count = lax.axis_size(axis)
    return lax.ppermute(value, axis, [(i, i ^ step) for i in range(count)])


def bits_of(count):
    return [1 << t for t in range(count.bit_length() - 1)]


class Stream:
    def __init__(self, matrix, buffer, sems, window, steps):
        self.matrix, self.buffer, self.sems = matrix, buffer, sems
        self.window, self.steps, self.depth = window, steps, buffer.shape[0]
        self.shape = buffer.shape[2:]

    def copy(self, step):
        row, column = self.window(step)
        slot = lax.rem(step, self.depth) if not isinstance(step, int) else step % self.depth
        rows, columns = self.shape
        if not isinstance(step, int):
            row, column = pl.multiple_of(row, rows), pl.multiple_of(column, LANES)
        source = self.matrix.at[:, pl.ds(row, rows), pl.ds(column, columns)]
        return pltpu.make_async_copy(source, self.buffer.at[slot], self.sems.at[slot])

    def begin(self):
        for step in range(min(self.depth, self.steps)):
            self.copy(step).start()

    def run(self, compute):
        @pl.loop(0, self.steps)
        def _(step):
            self.copy(step).wait()
            compute(step, self.buffer.at[lax.rem(step, self.depth)])

            @pl.when(step + self.depth < self.steps)
            def _():
                self.copy(step + self.depth).start()


def ring(tile, count):
    depth = min(DEPTH, count)
    return [pltpu.VMEM((depth, 2, *tile), F32), pltpu.SemaphoreType.DMA((depth,))]


def first_factor(vectors, half):
    rows, width = vectors.shape

    def kernel(v_ref, real_ref, imag_ref):
        value = v_ref[...]
        real_ref[...] = stack_split(value)
        imag_ref[...] = stack_split(twisted(value, half, 1.0))

    shape = jax.ShapeDtypeStruct((2 * rows, width), BF16)
    return pl.pallas_call(kernel, out_shape=(shape, shape), name="first_factor")(vectors)


def column_product(coupling, real_factor, imag_factor, chunk, width, bits):
    double, height = real_factor.shape
    rows = double // 2
    order = offsets(bits)
    members = len(order)
    piece = width // members
    tile = (min(COLUMN_TILE[0], height), min(COLUMN_TILE[1], width))
    down, along = height // tile[0], width // tile[1]
    steps = down * along

    def kernel(h_ref, real_ref, imag_ref, near_ref, far_ref, total, pieces, buffer, sems):
        def window(step):
            return (step % down) * tile[0], chunk * width + (step // down) * tile[1]

        stream = Stream(h_ref, buffer, sems, window, steps)
        stream.begin()
        total[...] = jnp.zeros_like(total)

        def compute(step, matrix):
            inner = pl.ds(pl.multiple_of(lax.rem(step, down) * tile[0], tile[0]), tile[0])
            outer = pl.ds(pl.multiple_of(lax.div(step, down) * tile[1], tile[1]), tile[1])
            total[:, outer] += block_product(matrix, real_ref[:, inner], imag_ref[:, inner], NN)

        stream.run(compute)
        mine = lax.axis_index("rows")
        for p in range(members):
            pieces[p] = total[:, p * piece : (p + 1) * piece]
        for e in range(members // 2):
            near_ref[e] = pieces[mine ^ order[e]]
            far_ref[e] = pieces[mine ^ order[members // 2 + e]]

    out = jax.ShapeDtypeStruct((members // 2, rows, piece), F32)
    vmem = pl.BlockSpec(memory_space=pltpu.VMEM)
    return pl.pallas_call(
        kernel,
        in_specs=[ANY, vmem, vmem],
        out_shape=[out, out],
        scratch_shapes=[
            pltpu.VMEM((rows, width), F32),
            pltpu.VMEM((members, rows, piece), F32),
            *ring(tile, steps),
        ],
        name="column_product",
        cost_estimate=pl.CostEstimate(
            flops=4 * 3 * rows * height * width,
            bytes_accessed=8 * height * width,
            transcendentals=0,
        ),
    )(coupling, real_factor, imag_factor)


def sum_all(parts):
    return functools.reduce(jnp.add, parts)


def prepare(parts, bits, inverse, before, carry, extra, chunk, width, geometry):
    rows_axis, cols_axis, chunks = geometry
    order = offsets(bits)
    _, rows, piece = parts[0].shape
    half = rows // 2
    height = before.shape[1]
    first = carry is None
    normal = inverse is not None
    start = chunk * width
    owner_row, offset = start // height, start % height
    kept = height // cols_axis
    per_chunk = width // kept
    ratio = rows_axis // cols_axis

    def kernel(*refs):
        refs = list(refs)
        part_refs = [refs.pop(0) for _ in parts]
        inverse_ref = refs.pop(0) if normal else None
        before_ref = refs.pop(0)
        carry_refs = None if first else [refs.pop(0) for _ in range(2)]
        extra_ref = None if extra is None else refs.pop(0)
        real_ref, imag_ref, small_ref, keep_ref, vector_ref, pieces = refs
        gram_ref, cross_ref = small_ref.at[:half], small_ref.at[half : 2 * half]
        row, column = lax.axis_index("rows"), lax.axis_index("cols")
        split_at = len(order) // len(parts)
        for e, k in enumerate(order):
            pieces[row ^ k] = part_refs[e // split_at][e % split_at]
        value = jnp.concatenate([pieces[p] for p in range(rows_axis)], axis=1)
        if normal:
            value = triple(inverse_ref[...], value, NN)
        vector_ref[...] = value
        factor = stack_split(value)
        real_ref[...] = factor
        imag_ref[...] = stack_split(twisted(value, half, -1.0))
        gram = pairs(factor, factor, half)
        ours = (row == column * ratio + owner_row).astype(F32)
        earlier = stack_split(before_ref[:, offset : offset + width])
        cross = pairs(earlier, factor, half) * ours
        gram_ref[...] = gram if first else carry_refs[0][:half] + gram
        cross_ref[...] = cross if first else carry_refs[0][half:] + cross
        if extra is not None:
            small_ref[2 * half :] = extra_ref[...]
        keep_ref[...] = jnp.zeros_like(keep_ref) if first else carry_refs[1][...]
        for p in range(per_chunk):

            @pl.when(row == chunk * per_chunk + p)
            def _(p=p):
                keep_ref[...] = vector_ref[:, p * kept : (p + 1) * kept]

    below = 0 if extra is None else extra.shape[0]
    factor = jax.ShapeDtypeStruct((2 * rows, width), BF16)
    operands = [*parts]
    operands += [inverse] if normal else []
    operands += [before]
    operands += [] if first else list(carry)
    operands += [] if extra is None else [extra]
    real, imag, small, keep, vectors = pl.pallas_call(
        kernel,
        out_shape=[
            factor,
            factor,
            jax.ShapeDtypeStruct((2 * half + below, LANES), F32),
            jax.ShapeDtypeStruct((rows, kept), F32),
            jax.ShapeDtypeStruct((rows, width), F32),
        ],
        scratch_shapes=[pltpu.VMEM((rows_axis, rows, piece), F32)],
        name="prepare",
    )(*operands)
    return (real, imag), (small, keep), vectors


def row_product(coupling, factors, carry, chunk, geometry):
    _, cols_axis, chunks = geometry
    double, width = factors[0].shape
    rows = double // 2
    height = coupling.shape[1]
    first, last = carry is None, chunk == chunks - 1
    start = chunk * width
    kept = height // cols_axis
    tile = (min(ROW_TILE[0], height), min(ROW_TILE[1], width))
    down, along = height // tile[0], width // tile[1]
    steps = down * along
    n_sum = 2 if last else 1

    def kernel(*refs):
        refs = list(refs)
        h_ref, real_ref, imag_ref = (refs.pop(0) for _ in range(3))
        carry_ref = None if first else refs.pop(0)
        sum_refs = [refs.pop(0) for _ in range(n_sum)]
        buffer, sems = refs.pop(0), refs.pop(0)
        total, out_pieces = refs if last else (sum_refs[0], None)
        column = lax.axis_index("cols")

        def window(step):
            return (step // along) * tile[0], start + (step % along) * tile[1]

        stream = Stream(h_ref, buffer, sems, window, steps)
        stream.begin()
        if along > 1:
            total[...] = jnp.zeros_like(total) if first else carry_ref[...]

        def compute(step, matrix):
            inner = pl.ds(pl.multiple_of(lax.rem(step, along) * tile[1], tile[1]), tile[1])
            outer = pl.ds(pl.multiple_of(lax.div(step, along) * tile[0], tile[0]), tile[0])
            part = block_product(matrix, real_ref[:, inner], imag_ref[:, inner], NT)
            if along > 1:
                total[:, outer] += part
            else:
                total[:, outer] = part if first else carry_ref[:, outer] + part

        stream.run(compute)
        if last:
            for p in range(cols_axis):
                out_pieces[p] = total[:, p * kept : (p + 1) * kept]
            for e in range(cols_axis // 2):
                sum_refs[0][e] = out_pieces[column ^ (2 * e)]
                sum_refs[1][e] = out_pieces[column ^ (2 * e + 1)]

    pair = jax.ShapeDtypeStruct((cols_axis // 2, rows, kept), F32)
    out_shape = [pair, pair] if last else [jax.ShapeDtypeStruct((rows, height), F32)]
    scratch = ring(tile, steps)
    if last:
        scratch += [pltpu.VMEM((rows, height), F32), pltpu.VMEM((cols_axis, rows, kept), F32)]
    operands = [*factors] + ([] if first else [carry])
    outs = pl.pallas_call(
        kernel,
        in_specs=[ANY] + [pl.BlockSpec(memory_space=pltpu.VMEM)] * len(operands),
        out_shape=out_shape,
        scratch_shapes=scratch,
        name="row_product",
        cost_estimate=pl.CostEstimate(
            flops=4 * 3 * rows * height * width,
            bytes_accessed=8 * height * width,
            transcendentals=0,
        ),
    )(coupling, *operands)
    return outs if last else outs[0]


def inverse_factor(parts, count, order):
    total_rows = parts[0].shape[0]
    middle = LANES // 2
    rest = total_rows - count

    def kernel(*refs):
        ins, outs = refs[: len(parts)], refs[len(parts) :]
        total = sum_all([ref[...] for ref in ins])
        if rest:
            outs[1][...] = total[count:]
        gram = total[:count] * (1.0 / order)
        lane = lax.broadcasted_iota(jnp.int32, (count, LANES), 1)
        row = lax.broadcasted_iota(jnp.int32, (count, LANES), 0)
        left = lane < count
        identity = (lane == row + middle).astype(F32)
        real = jnp.where(left, gram, identity)
        imag = jnp.where(left, pltpu.roll(gram, middle, 1), 0.0)
        row_column = lax.broadcasted_iota(jnp.int32, (count, 1), 0)
        scale = jnp.zeros((count, 1), F32)
        for j in range(count):
            pivot = real[j : j + 1, j : j + 1]
            scale = jnp.where(row_column == j, lax.rsqrt(pivot), scale)
            if j == count - 1:
                break
            top = (j + 1) // 8 * 8
            below = row_column[top:] > j
            gain = 1.0 / pivot
            column_real = jnp.where(below, real[top:, j : j + 1] * gain, 0.0)
            column_imag = jnp.where(below, imag[top:, j : j + 1] * gain, 0.0)
            row_real, row_imag = real[j : j + 1], imag[j : j + 1]
            new_real = real[top:] - (column_real * row_real - column_imag * row_imag)
            new_imag = imag[top:] - (column_real * row_imag + column_imag * row_real)
            real = jnp.concatenate([real[:top], new_real], axis=0) if top else new_real
            imag = jnp.concatenate([imag[:top], new_imag], axis=0) if top else new_imag
        real = (real * scale)[:, middle : middle + count]
        imag = (imag * scale)[:, middle : middle + count]
        outs[0][...] = jnp.concatenate(
            [
                jnp.concatenate([real, -imag], axis=1),
                jnp.concatenate([imag, real], axis=1),
            ],
            axis=0,
        )

    out_shape = [jax.ShapeDtypeStruct((2 * count, 2 * count), F32)]
    if rest:
        out_shape.append(jax.ShapeDtypeStruct((rest, LANES), F32))
    outs = pl.pallas_call(kernel, out_shape=out_shape, name="inverse_factor")(*parts)
    return (outs[0], outs[1] if rest else None)


def next_factor(own, inverse, earlier, extra, geometry):
    rows_axis, cols_axis, chunks = geometry
    _, rows, kept = own[0][0].shape
    half = rows // 2
    height = kept * cols_axis
    width = earlier[0].shape[1]
    ratio = rows_axis // cols_axis
    counts = [len(terms) for terms in own]
    flat = [term for terms in own for term in terms]

    def kernel(*refs):
        refs = list(refs)
        term_refs = [[refs.pop(0) for _ in range(n)] for n in counts]
        inverse_ref = refs.pop(0)
        earlier_refs = [refs.pop(0) for _ in range(chunks)]
        extra_ref, real_ref, imag_ref, value_ref, small_ref, pieces, packed = refs
        gram_ref, cross_ref = small_ref.at[:half], small_ref.at[half : 2 * half]
        small_ref[2 * half :] = extra_ref[...]
        row, column = lax.axis_index("rows"), lax.axis_index("cols")
        for k in range(cols_axis):
            terms = [ref[(k // 2) ^ m] for m, ref in enumerate(term_refs[k % 2])]
            pieces[column ^ k] = sum_all(terms)
        value = jnp.concatenate([pieces[p] for p in range(cols_axis)], axis=1)
        value = triple(inverse_ref[...], value, NN)
        value_ref[...] = value
        factor = stack_split(value)
        packed[...] = factor
        real_ref[...] = factor
        imag_ref[...] = stack_split(twisted(value, half, 1.0))
        gram_ref[...] = pairs(factor, factor, half)
        cross_ref[...] = jnp.zeros_like(cross_ref)
        for j in range(chunks):
            owner, offset = j * width // height, j * width % height

            @pl.when(row == column * ratio + owner)
            def _(j=j, offset=offset):
                cross_ref[...] += pairs(
                    stack_split(earlier_refs[j][...]),
                    packed[:, offset : offset + width],
                    half,
                )

    factor_shape = jax.ShapeDtypeStruct((2 * rows, height), BF16)
    return pl.pallas_call(
        kernel,
        out_shape=[
            factor_shape,
            factor_shape,
            jax.ShapeDtypeStruct((rows, height), F32),
            jax.ShapeDtypeStruct((2 * half + extra.shape[0], LANES), F32),
        ],
        scratch_shapes=[
            pltpu.VMEM((cols_axis, rows, kept), F32),
            pltpu.VMEM((2 * rows, height), BF16),
        ],
        name="next_factor",
    )(*flat, inverse, *earlier, extra)


def last_vectors(terms, inverse, earlier, extra, share):
    rows, kept = terms[0].shape
    half = rows // 2

    def kernel(*refs):
        ins, (inverse_ref, earlier_ref, extra_ref, value_ref, both_ref) = refs[: len(terms)], refs[len(terms) :]
        value = triple(inverse_ref[...], sum_all([ref[...] for ref in ins]), NN)
        value_ref[...] = value
        factor = stack_split(value)
        both_ref[:half] = pairs(factor, factor, half)
        both_ref[half : 2 * half] = pairs(stack_split(earlier_ref[...]), factor, half)
        both_ref[2 * half :] = extra_ref[...] * share

    return pl.pallas_call(
        kernel,
        out_shape=[
            jax.ShapeDtypeStruct((rows, kept), F32),
            jax.ShapeDtypeStruct((3 * half, LANES), F32),
        ],
        name="last_vectors",
    )(*terms, inverse, earlier, extra)


def finish(value, inverse, crosses, inverses, order):
    rows, kept = value.shape
    half = rows // 2
    middle = LANES // 2
    count = len(crosses)

    def kernel(*refs):
        value_ref, inverse_ref = refs[:2]
        cross_refs, inverse_refs = refs[2 : 2 + count], refs[2 + count : 1 + 2 * count]
        basis_ref, ritz_ref = refs[1 + 2 * count :]
        result = triple(inverse_ref[...], value_ref[...], NN)
        basis_ref[0], basis_ref[1] = result[:half], result[half:]
        for t in range(count):
            cross = cross_refs[t][...] * (1.0 / order)
            stacked = jnp.concatenate(
                [cross[:, :half], cross[:, middle : middle + half]], axis=0
            )
            if t:
                factor = inverse_refs[t - 1][...]
                conjugate = jnp.concatenate(
                    [
                        jnp.concatenate([factor[:half, :half], -factor[:half, half:]], axis=1),
                        jnp.concatenate([-factor[half:, :half], factor[half:, half:]], axis=1),
                    ],
                    axis=0,
                )
                stacked = triple(conjugate, stacked, NN)
            ritz_ref[t, 0], ritz_ref[t, 1] = stacked[:half], stacked[half:]

    return pl.pallas_call(
        kernel,
        out_shape=[
            jax.ShapeDtypeStruct((2, half, kept), F32),
            jax.ShapeDtypeStruct((count, 2, half, half), F32),
        ],
        name="finish",
    )(value, inverse, *crosses, *inverses)


def body(coupling, initial):
    rows_axis, cols_axis = lax.axis_size("rows"), lax.axis_size("cols")
    half = initial.shape[1]
    rows = 2 * half
    height, span = coupling.shape[1], coupling.shape[2]
    order = float(height * rows_axis)
    ratio = rows_axis // cols_axis
    chunks = max(ratio, CHUNKS)
    width = span // chunks
    geometry = (rows_axis, cols_axis, chunks)
    row_bits, col_bits = bits_of(rows_axis), bits_of(cols_axis)
    orders = [row_bits] * chunks

    def tie(value, after):
        return lax.optimization_barrier((value, after))

    def forward(real_factor, imag_factor, small):
        steps = list(row_bits)
        products = []
        for chunk in range(chunks):
            if small is not None:
                now = steps if chunk == chunks - 1 else steps[:1]
                steps = steps[len(now) :]
                came = [exchange(small, "rows", k) for k in offsets(now)[1:]]
                if len(now) > 2 or chunk == chunks - 1 and len(came) > 3:
                    came, steps = came[:0], now
            products.append(
                column_product(coupling, real_factor, imag_factor, chunk, width, orders[chunk])
            )
            if chunk + 1 < chunks:
                if small is not None:
                    small = sum_all([small, *came])
                    real_factor, small = tie(real_factor, small)
            elif small is not None:
                small = sum_all([small, *came])
        for step in steps if small is not None else []:
            small = small + exchange(small, "rows", step)
        inverse = rest = None
        nears = [near for near, _ in products]
        nears = list(lax.optimization_barrier(tuple(nears)))
        fars = [far for _, far in products]
        came = [exchange(far, "rows", bits[0]) for far, bits in zip(fars, orders)]
        length = 2 * len(row_bits) - 1
        turns = sorted(
            (turn + 1.5 * chunk, chunk, turn) for chunk in range(chunks) for turn in range(length)
        )
        done = None
        for _, chunk, turn in turns:
            bits, near, here = orders[chunk], nears[chunk], came[chunk]
            if done is not None:
                near, done = tie(near, done)
            if turn < len(bits) - 1:
                middle = near.shape[0] // 2
                nears[chunk] = near[:middle] + here[:middle]
                came[chunk] = exchange(near[middle:] + here[middle:], "rows", bits[turn + 1])
            elif turn == len(bits) - 1:
                nears[chunk] = near + here
                came[chunk] = exchange(nears[chunk], "rows", bits[turn])
            else:
                nears[chunk] = jnp.concatenate([near, here], axis=0)
                came[chunk] = exchange(nears[chunk], "rows", bits[2 * len(bits) - 2 - turn])
            done = nears[chunk]
            if small is not None and inverse is None:
                small, done = tie(small, done)
                inverse, rest = inverse_factor([small], half, order)
                done = inverse
        gathered = [[near, here] for near, here in zip(nears, came)]
        return gathered, inverse, rest

    def backward(gathered, inverse, before, extra):
        carry, vectors, sums = None, [], None
        steps = list(col_bits)
        for chunk in range(chunks):
            parts = gathered[chunk]
            if sums is not None:
                parts, sums = tie(parts, sums)
            below = extra if chunk == chunks - 1 else None
            factors, carry, value = prepare(
                parts, orders[chunk], inverse, before, carry, below, chunk, width, geometry
            )
            vectors.append(value)
            away = None
            if chunk == chunks - 1:
                small, keep = carry
                away = exchange(small, "cols", steps.pop(0))
            sums = row_product(coupling, factors, sums, chunk, geometry)
        small = small + away
        while steps:
            small = small + exchange(small, "cols", steps.pop(0))
        near, far = sums
        near = near + exchange(far, "cols", 1)
        near, small = tie(near, small)
        return near, small, keep, vectors

    def total(value, axis, bits):
        for bit in bits:
            value = value + exchange(value, axis, bit)
        return value

    start = initial.reshape(rows, height)
    real_factor, imag_factor = first_factor(start, half)
    others = range(2, cols_axis, 2)
    gathered, _, _ = forward(real_factor, imag_factor, None)
    near, packed, _, vectors = backward(gathered, None, start, None)
    across = [exchange(near, "cols", m) for m in others]
    inverse_1, cross_1 = inverse_factor([packed], half, order)
    across, inverse_1 = tie(tuple(across), inverse_1)
    across = [near, *across]
    own = [across, [exchange(term, "cols", 1) for term in across]]
    real_factor, imag_factor, before, packed = next_factor(own, inverse_1, vectors, cross_1, geometry)
    gathered, inverse_2, crosses = forward(real_factor, imag_factor, packed)
    cross_2, cross_1 = crosses[:half], crosses[half:]
    near, packed, keep, _ = backward(gathered, inverse_2, before, cross_2)
    keep = lax.ppermute(
        keep,
        ("rows", "cols"),
        [
            (r * cols_axis + c, (c * ratio + r // cols_axis) * cols_axis + r % cols_axis)
            for r in range(rows_axis)
            for c in range(cols_axis)
        ],
    )
    terms = [near[0]] + [exchange(near[m // 2], "cols", m) for m in others]
    inverse_3, crosses = inverse_factor([packed], half, order)
    cross_3, cross_2 = crosses[:half], crosses[half:]
    value, packed = last_vectors(terms, inverse_3, keep, cross_3, 1.0 / cols_axis)
    packed = total(total(packed, "cols", col_bits), "rows", row_bits)
    inverse_4, crosses = inverse_factor([packed], half, order)
    cross_4, cross_3 = crosses[:half], crosses[half:]
    return tuple(
        finish(
            value,
            inverse_4,
            [cross_1, cross_2, cross_3, cross_4],
            [inverse_1, inverse_2, inverse_3],
            order,
        )
    )


def solution(mesh):
    return jax.shard_map(
        body,
        mesh=mesh,
        in_specs=(P(None, "rows", "cols"), P(None, None, "rows")),
        out_specs=(P(None, None, ("rows", "cols")), P()),
        check_vma=False,
    )
```
